32 devices in a mesh: row: 4 (over z), col: 8 (over y, x, core).
Axes of the slice: x: 2, y: 2, z: 4, core: 2. Of those that a mesh axis runs over, the one named last changes fastest.
Arguments:
- point_coords: float32 [1024, 3, 256], P(('row', 'col')), may hold values from 0 to 10
- fluid_force: float32 [1024, 3, 256], P(('row', 'col')), may hold values from -6 to 6
- tile_clusters: int32 [1024, 8], P(('row', 'col')), may hold values from 0 to 511, as said below
- pu_level: int32 [1024, 8, 256], P(('row', 'col')), may hold values from 0 to 15
- node_coords: float32 [512, 3, 512], P(('row', 'col')), may hold values from 0 to 10
- node_disp: float32 [512, 3, 512], P(('row', 'col')), may hold values from -6 to 6
- inverse: float32 [512, 512, 512], P(('row', 'col')), may hold values from -0.25 to 0.25
Outputs:
- point_disp: float32 [1024, 3, 256], P(('row', 'col'))
- node_force: float32 [512, 3, 512], P(('row', 'col'))
The draws below stay inside these ranges and needn't reach their ends.
Inputs may be any that keep to these rules, and one draw needn't show every extreme that they name: `tile_clusters`: cluster c lives with rows c of the cluster arrays; tile t's k-th entry names a cluster intersecting it, possibly more than once in a tile. Among the 256 entries of one device's tiles, at most 8 name clusters of any one device (clusters d * 16 to d * 16 + 15).
All inputs are finite; a program needn't handle non-finite values.
Results may differ from the reference program's by a relative error of at most 0.0003.
Values sent between devices are 32-bit elements; how exact they have to be, the bound alone decides.
No kernel may reach another device: no remote copies, remote signals or barrier semaphores. Data moves between devices by JAX's collectives and lax.ppermute only.
A program may use at most 128 MiB of HBM per device.

```python
import jax
import jax.numpy as jnp
from jax import lax

NODES = 512
TILE = 256
KMAX = 8
CAP = 8
CL_DEV = 16
TILE_DEV = 32
CLUSTERS = 512
TILES = 1024
N_ROW = 4
N_COL = 8


def tile_ids(key):
    dev_total = N_ROW * N_COL
    slot_total = dev_total * CAP
    pair_total = TILE_DEV * KMAX
    heat_level = jax.random.randint(jax.random.fold_in(key, 1), (dev_total,), 0, 4)
    hot_owner = jax.random.randint(jax.random.fold_in(key, 2), (), 0, dev_total)
    owner_of = jnp.arange(slot_total) // CAP
    base_score = jax.random.randint(jax.random.fold_in(key, 3), (dev_total, slot_total), 0, 512)
    scores = base_score + heat_level[owner_of][None, :] * 512 + jnp.where(owner_of == hot_owner, 8192, 0)[None, :]
    breakers = jax.vmap(lambda sub: jax.random.permutation(sub, slot_total))(jax.random.split(jax.random.fold_in(key, 4), dev_total))
    scores = scores * slot_total + breakers
    unused, chosen = lax.top_k(scores, pair_total)
    shuffles = jax.vmap(lambda sub: jax.random.permutation(sub, pair_total))(jax.random.split(jax.random.fold_in(key, 5), dev_total))
    chosen = jnp.take_along_axis(chosen, shuffles, axis=1)
    local_id = jax.random.randint(jax.random.fold_in(key, 6), (dev_total, pair_total), 0, CL_DEV)
    cluster_ids = chosen // CAP * CL_DEV + local_id
    return cluster_ids.reshape(dev_total * TILE_DEV, KMAX).astype(jnp.int32)


def cluster_centres(key):
    return jax.random.uniform(jax.random.fold_in(key, 20), (CLUSTERS, 3), jnp.float32, 1.0, 9.0)


def draw_tile_clusters(key, part):
    return tile_ids(key)


def draw_node_coords(key, part):
    centre = cluster_centres(key)
    half_width = jnp.array([0.5, 0.5, 0.5], jnp.float32)
    spread = jax.random.uniform(jax.random.fold_in(key, 21), (CLUSTERS, 3, NODES), jnp.float32, -1.0, 1.0)
    return (centre[:, :, None] + spread * half_width[None, :, None]).astype(jnp.float32)


def draw_point_coords(key, part):
    cluster_ids = tile_ids(key)
    centre = cluster_centres(key)
    pick = jax.random.randint(jax.random.fold_in(key, 22), (TILES, TILE), 0, KMAX)
    nearest = jnp.take_along_axis(cluster_ids, pick, axis=1)
    base = jnp.transpose(centre[nearest], (0, 2, 1))
    half_width = jnp.array([0.75, 0.75, 0.75], jnp.float32)
    spread = jax.random.uniform(jax.random.fold_in(key, 23), (TILES, 3, TILE), jnp.float32, -1.0, 1.0)
    return (base + spread * half_width[None, :, None]).astype(jnp.float32)


def touch_ends(values, key, smallest, top_value):
    longest = values.shape.index(max(values.shape))
    spots = []
    for shift in (0, 1):
        where = [jax.random.randint(jax.random.fold_in(key, axis), (), 0, length) for axis, length in enumerate(values.shape)]
        where[longest] = (where[longest] + shift) % values.shape[longest]
        spots.append(tuple(where))
    return values.at[spots[0]].set(smallest).at[spots[1]].set(top_value)


def block_levels(own_key, shape, cuts, smallest, top_value):
    def one(position, parts):
        heights = jax.random.uniform(jax.random.fold_in(jax.random.fold_in(own_key, 6), position), (parts,), jnp.float32, smallest / len(cuts), top_value / len(cuts))
        return jnp.repeat(jnp.exp(heights), shape[position] // parts).reshape((-1,) + (1,) * (len(shape) - position - 1))

    loudness = one(*cuts[0])
    for cut in cuts[1:]:
        loudness = loudness * one(*cut)
    return loudness


def noise(rng, shape, deviation, limit, cuts=(), kind=jnp.bfloat16):
    drawn = deviation * jax.random.normal(rng, shape, jnp.float32)
    if cuts:
        drawn = drawn * block_levels(rng, shape, cuts, -0.22, 0.18)
    return jnp.clip(drawn, -limit, limit).astype(kind)


def setup_inputs(seed: int = 0) -> dict:
    splits = jax.random.split(jax.random.key(seed), 8)
    return {
        "point_coords": draw_point_coords(jax.random.fold_in(splits[7], 71), 0),
        "fluid_force": noise(splits[1], (TILES, 3, TILE), 1.0, 6.0, ((0, 32),), jnp.float32),
        "tile_clusters": draw_tile_clusters(jax.random.fold_in(splits[7], 71), 0),
        "pu_level": touch_ends(jax.random.randint(splits[3], (TILES, KMAX, TILE), 0, 16), jax.random.fold_in(splits[3], 1), 0, 15).astype(jnp.int32),
        "node_coords": draw_node_coords(jax.random.fold_in(splits[7], 71), 0),
        "node_disp": noise(splits[5], (CLUSTERS, 3, NODES), 1.0, 6.0, ((0, 32),), jnp.float32),
        "inverse": noise(splits[6], (CLUSTERS, NODES, NODES), NODES ** -0.5, 0.25, ((0, 32),), jnp.float32),
    }


def kernel(points, node_rows):
    offset = points[..., :, :, None] - node_rows[..., :, None, :]
    scaled = jnp.sqrt(lax.optimization_barrier(jnp.sum(offset * offset, axis=-3)))
    return jnp.maximum(1.0 - scaled, 0.0) ** 4 * (4.0 * scaled + 1.0)

def reference(point_coords, fluid_force, tile_clusters, pu_level, node_coords, node_disp, inverse):
    highest = lax.Precision.HIGHEST
    coeffs = jnp.einsum('cin,cnm->cim', node_disp, inverse, precision=highest)
    levels = pu_level.astype(jnp.float32) + 1.0
    weights = levels / lax.optimization_barrier(jnp.sum(levels, axis=1, keepdims=True))

    def per_tile(force_sum, bundle):
        cluster_ids, points, tile_force, weight = bundle
        kernel_vals = kernel(points[None], node_coords[cluster_ids])
        values = jnp.einsum('kpn,kin->kip', kernel_vals, coeffs[cluster_ids], precision=highest)
        shown_disp = lax.optimization_barrier(jnp.sum(weight[:, None, :] * values, axis=0))
        loads = weight[:, None, :] * tile_force[None]
        partial_value = jnp.einsum('kpn,kip->kin', kernel_vals, loads, precision=highest)
        return (force_sum.at[cluster_ids].add(partial_value), shown_disp)
    empty_sum = jnp.zeros(node_coords.shape, jnp.float32)
    node_force, point_disp = lax.scan(per_tile, empty_sum, (tile_clusters, point_coords, fluid_force, weights))
    return (point_disp, node_force)
```

```python
import functools

import jax
import jax.numpy as jnp
from jax import lax
from jax.experimental import pallas as pl
from jax.experimental.pallas import tpu as pltpu
from jax.sharding import PartitionSpec as P

CAP = 8
BATCH = 128
CHUNK = 256
WINDOW = 64
AXES = ("row", "col")
FAR = 1e9
NT = (((1,), (1,)), ((), ()))
F32 = jnp.float32
BF16 = jnp.bfloat16


def rounded(x):
    return x.astype(BF16).astype(F32)


def split2(x):
    high = rounded(x)
    return high, rounded(x - high)


def split3(x):
    high = rounded(x)
    rest = x - high
    middle = rounded(rest)
    return high, middle, rounded(rest - middle)


def outer_split(x, parts):
    pieces = []
    for _ in range(parts):
        piece = lax.reduce_precision(x, 8, 7)
        pieces.append(piece)
        x = x - piece
    return pieces


def tile_weights(levels):
    levels = levels.astype(F32) + 1.0
    return levels / jnp.sum(levels, axis=0, keepdims=True)


def pack_kernel(local_count, full, ids, points, force, level, out, wanted, slot_of, count):
    devices = out.shape[0]
    tiles, kslots = level.shape[0], level.shape[1]

    @pl.loop(0, devices)
    def _(d):
        count[d] = 0

    if not full:

        @pl.loop(0, devices)
        def _(d):
            out[d] = jnp.zeros(out.shape[1:], F32)
            for j in range(CAP):
                wanted[d * CAP + j] = -1

    @pl.loop(0, tiles)
    def _(t):
        weights = tile_weights(level[t])
        coords = [points[c, pl.ds(t, 1), :] for c in range(3)]
        loads = [weights * (force[c, pl.ds(t, 1), :] * (1.0 / 256.0)) for c in range(3)]
        for k in range(kslots):
            pair = t * kslots + k
            cluster = ids[pair]
            d = cluster // local_count
            j = count[d]
            count[d] = j + 1
            wanted[d * CAP + j] = cluster - d * local_count
            slot_of[pair] = d * CAP + j
            for c in range(3):
                out[d, pl.ds(c * CAP + j, 1), :] = coords[c]
                out[d, pl.ds((3 + c) * CAP + j, 1), :] = loads[c][k : k + 1]


def unpack_kernel(slot_of, back, level, out):
    tiles, kslots = level.shape[0], level.shape[1]

    @pl.loop(0, tiles)
    def _(t):
        weights = tile_weights(level[t])
        sums = [None] * 3
        for k in range(kslots):
            slot = slot_of[t * kslots + k]
            d = slot // CAP
            j = slot - d * CAP
            for c in range(3):
                term = weights[k : k + 1] * back[d, pl.ds(c * CAP + j, 1), :]
                sums[c] = term if k == 0 else sums[c] + term
        for c in range(3):
            out[c, pl.ds(t, 1), :] = sums[c]


def couple_kernel(
    ids,
    boxes,
    arrived,
    node_rows,
    coeff_rows,
    values,
    node_force,
    rank,
    rows,
    packed,
    slot_plan_v,
    cluster_plan_v,
    slot_plan,
    cluster_plan,
    force_sum,
    sems,
):
    groups = arrived.shape[0]
    width = arrived.shape[2]
    batch = groups * CAP
    clusters = node_rows.shape[0]
    step = pl.program_id(0)

    @pl.when(step == 0)
    def _():
        force_sum[...] = jnp.zeros_like(force_sum)

    @pl.loop(0, groups)
    def _(g):
        box = boxes[pl.ds(pl.multiple_of(g * CAP, CAP), CAP), :]
        gap = None
        for c in range(3):
            x = arrived[g, c * CAP : (c + 1) * CAP, :]
            side = jnp.maximum(jnp.maximum(box[:, c : c + 1] - x, x - box[:, 3 + c : 4 + c]), 0.0)
            gap = side * side if c == 0 else gap + side * side
        rank[pl.ds(pl.multiple_of(g * CAP, CAP), CAP), :] = jnp.where(gap < 1.0002, 1.0, 0.0)

    near = rank[...].astype(BF16)
    before = (
        lax.broadcasted_iota(jnp.int32, (width, width), 0)
        < lax.broadcasted_iota(jnp.int32, (width, width), 1)
    ).astype(F32).astype(BF16)
    earlier = jnp.dot(near, before, preferred_element_type=F32)
    rank[...] = jnp.where(near.astype(F32) > 0.5, earlier, -1e6)
    counts = lax.dot_general(jnp.ones((CAP, width), BF16), near, NT, preferred_element_type=F32)
    hits = (lax.broadcasted_iota(jnp.int32, (clusters, batch), 0) == ids[0]).astype(F32)
    hit_counts = hits * counts[0:1]
    before_slot = (
        lax.broadcasted_iota(jnp.int32, (batch, batch), 0)
        < lax.broadcasted_iota(jnp.int32, (batch, batch), 1)
    ).astype(F32).astype(BF16)
    slot_start = jnp.dot(hit_counts.astype(BF16), before_slot, preferred_element_type=F32)
    totals = jnp.sum(hit_counts, axis=1, keepdims=True)
    chunks = jnp.floor((totals + (CHUNK - 1)) * (1.0 / CHUNK))
    chunks = jnp.broadcast_to(chunks, (clusters, 128))
    before_cluster = (
        lax.broadcasted_iota(jnp.int32, (clusters, clusters), 1)
        < lax.broadcasted_iota(jnp.int32, (clusters, clusters), 0)
    ).astype(F32).astype(BF16)
    first_chunk = jnp.dot(before_cluster, chunks.astype(BF16), preferred_element_type=F32)
    offset = jnp.sum(hits * (slot_start + first_chunk[:, 0:1] * CHUNK), axis=0, keepdims=True)
    slot_plan_v[0:1, :] = offset.astype(jnp.int32)
    slot_plan_v[1:2, :] = counts[0:1].astype(jnp.int32)
    lane = lax.broadcasted_iota(jnp.int32, (clusters, 128), 1)
    cluster_plan_v[...] = jnp.where(lane == 0, first_chunk, chunks).astype(jnp.int32)
    copies = [
        pltpu.make_async_copy(slot_plan_v, slot_plan, sems.at[0]),
        pltpu.make_async_copy(cluster_plan_v, cluster_plan, sems.at[1]),
    ]
    for copy in copies:
        copy.start()
    for copy in copies:
        copy.wait()
    total_chunks = cluster_plan[clusters - 1, 0] + cluster_plan[clusters - 1, 1]

    @pl.loop(0, total_chunks + 1)
    def _(j):
        packed[pl.ds(pl.multiple_of(j * CHUNK, CHUNK), CHUNK), :] = jnp.zeros((CHUNK, 128), F32)

    target = lax.broadcasted_iota(jnp.int32, (WINDOW, 1), 0).astype(F32)

    def place_of(g, i):
        slot = g * CAP + i
        start = slot_plan[0, slot]
        base = (start // 8) * 8
        lead = start - base
        blocks = (lead + slot_plan[1, slot] + (WINDOW - 1)) // WINDOW
        return rank[pl.ds(slot, 1), :], base, lead, blocks

    def selection(ranks, lead, block):
        shift = (lead - block * WINDOW).astype(F32)
        return jnp.where(ranks + shift == target, 1.0, 0.0).astype(BF16)

    def window_of(base, block):
        return pl.ds(pl.multiple_of(base + block * WINDOW, 8), WINDOW)

    @pl.loop(0, groups)
    def _(g):
        box = boxes[pl.ds(pl.multiple_of(g * CAP, CAP), CAP), :]
        x = [arrived[g, c * CAP : (c + 1) * CAP, :] - box[:, 6 + c : 7 + c] for c in range(3)]
        parts = [split3(v) for v in x]
        square = split3(x[0] * x[0] + x[1] * x[1] + x[2] * x[2])
        loads = [split2(arrived[g, (3 + c) * CAP : (4 + c) * CAP, :]) for c in range(3)]
        column = [parts[c][p] for p in (0, 1, 2, 0, 1, 0) for c in range(3)]
        column += list(square) + [jnp.ones_like(x[0])] * 3
        column += [loads[c][p] for p in range(2) for c in range(3)]
        column += [jnp.zeros_like(x[0])] * 2
        for i, tile in enumerate(column):
            rows[:, i * CAP : (i + 1) * CAP, :] = jnp.stack(
                [tile[:, h * 128 : (h + 1) * 128] for h in range(width // 128)]
            )
        places = [place_of(g, i) for i in range(CAP)]

        def slot_rows(i):
            return jnp.concatenate(
                [rows[h, pl.ds(i, 32, stride=CAP), :] for h in range(width // 128)], axis=1
            ).astype(BF16)

        moved = [
            lax.dot_general(
                selection(places[i][0], places[i][2], 0), slot_rows(i), NT, preferred_element_type=F32
            )
            for i in range(CAP)
        ]
        for i in range(CAP):
            packed[window_of(places[i][1], 0), 0:32] += moved[i]
        for i in range(CAP):
            ranks, base, lead, blocks = places[i]

            @pl.loop(1, blocks)
            def _(block):
                packed[window_of(base, block), 0:32] += lax.dot_general(
                    selection(ranks, lead, block), slot_rows(i), NT, preferred_element_type=F32
                )

    @pl.loop(0, clusters)
    def _(c):
        first = cluster_plan[c, 0]

        @pl.loop(0, cluster_plan[c, 1])
        def _(j):
            where = pl.ds(pl.multiple_of((first + j) * CHUNK, CHUNK), CHUNK)
            points = packed[where, :]
            square = jnp.dot(points[:, 0:32].astype(BF16), node_rows[c], preferred_element_type=F32)
            square = jnp.maximum(square, 1e-30)
            rest = jnp.maximum(4.0 - square * lax.rsqrt(square), 0.0)
            rest2 = rest * rest
            kernel = (rest2 * rest2) * (5.0 - rest)
            high = kernel.astype(BF16)
            low = (kernel - high.astype(F32)).astype(BF16)
            loads = jnp.transpose(points)[24:32].astype(BF16)
            packed[where, 0:16] = lax.dot_general(
                high, coeff_rows[c], NT, preferred_element_type=F32
            ) + lax.dot_general(low, coeff_rows[c], NT, preferred_element_type=F32)
            force_sum[c] += jnp.dot(loads, high, preferred_element_type=F32) + jnp.dot(
                loads, low, preferred_element_type=F32
            )

    @pl.loop(0, groups)
    def _(g):
        places = [place_of(g, i) for i in range(CAP)]

        def spread(place, block):
            ranks, base, lead, _ = place
            rows_t = jnp.transpose(packed[window_of(base, block), :])
            high, middle, low = split3(rows_t[0:8] + rows_t[8:16])
            stacked = jnp.concatenate([high, middle, low], axis=0).astype(BF16)
            moved = jnp.dot(stacked, selection(ranks, lead, block), preferred_element_type=F32)
            return moved[0:8] + moved[8:16] + moved[16:24]

        found = [spread(places[i], 0) for i in range(CAP)]
        for i in range(CAP):
            for c in range(3):
                values[g, c * CAP + i : c * CAP + i + 1, :] = found[i][c : c + 1]
        for i in range(CAP):

            @pl.loop(1, places[i][3])
            def _(block):
                more = spread(places[i], block)
                for c in range(3):
                    values[g, c * CAP + i : c * CAP + i + 1, :] += more[c : c + 1]

    @pl.when(step == pl.num_programs(0) - 1)
    def _():
        for c in range(clusters):
            both = force_sum[c]
            for i in range(3):
                node_force[i, c : c + 1, :] = both[i : i + 1] + both[3 + i : 4 + i]


def vmem():
    return pl.BlockSpec(memory_space=pltpu.VMEM)


def smem():
    return pl.BlockSpec(memory_space=pltpu.SMEM)


def on_device(point_coords, fluid_force, tile_clusters, pu_level, node_coords, node_disp, inverse):
    highest = lax.Precision.HIGHEST
    devices = lax.axis_size(AXES)
    slot_total = devices * CAP
    tile_total, kslots = tile_clusters.shape
    pair_total = tile_total * kslots
    local_count, _, node_count = node_coords.shape
    width = point_coords.shape[2]
    batch = min(BATCH, slot_total)
    groups = batch // CAP

    outgoing, wanted, slot_of = pl.pallas_call(
        functools.partial(pack_kernel, local_count, pair_total == slot_total),
        out_shape=(
            jax.ShapeDtypeStruct((devices, 6 * CAP, width), F32),
            jax.ShapeDtypeStruct((slot_total,), jnp.int32),
            jax.ShapeDtypeStruct((pair_total,), jnp.int32),
        ),
        in_specs=[smem(), vmem(), vmem(), vmem()],
        out_specs=(vmem(), smem(), smem()),
        scratch_shapes=[pltpu.SMEM((devices,), jnp.int32)],
        name="pack",
    )(
        tile_clusters.reshape(-1),
        jnp.transpose(point_coords, (1, 0, 2)),
        jnp.transpose(fluid_force, (1, 0, 2)),
        pu_level,
    )
    asked = lax.all_to_all(
        wanted.reshape(devices, CAP), AXES, split_axis=0, concat_axis=0, tiled=True
    ).reshape(slot_total)
    arrived = lax.all_to_all(outgoing, AXES, split_axis=0, concat_axis=0, tiled=True)

    coeffs = jnp.einsum("cin,cnm->cim", node_disp, inverse, precision=highest) * (1.0 / 256.0)
    high, low = outer_split(coeffs, 2)
    gap5 = jnp.zeros((local_count, 5, node_count), F32)
    coeff_rows = jnp.concatenate((high, gap5, low, gap5), axis=1).astype(BF16)
    least = jnp.min(node_coords, axis=2)
    most = jnp.max(node_coords, axis=2)
    centre = 0.5 * (least + most)
    nodes = node_coords - centre[:, :, None]
    near = [-32.0 * piece for piece in outer_split(nodes, 3)]
    square = [16.0 * p for p in outer_split(jnp.sum(nodes * nodes, axis=1, keepdims=True), 3)]
    sixteen = jnp.full((local_count, 3, node_count), 16.0, F32)
    rows = [near[0]] * 3 + [near[1]] * 2 + [near[2], sixteen] + square
    rows.append(jnp.zeros((local_count, 8, node_count), F32))
    node_rows = jnp.concatenate(rows, axis=1).astype(BF16)

    table = jnp.concatenate((least, most, centre), axis=1)
    chosen = asked[:, None] == jnp.arange(local_count, dtype=jnp.int32)[None, :]
    boxes = jnp.sum(jnp.where(chosen[:, :, None], table[None], 0.0), axis=1)
    nowhere = jnp.array([FAR] * 3 + [-FAR] * 3 + [0.0] * 3, F32)
    boxes = jnp.where(asked[:, None] < 0, nowhere[None], boxes)

    spare = local_count * CHUNK + CHUNK + 2 * WINDOW
    values, node_force = pl.pallas_call(
        couple_kernel,
        grid=(slot_total // batch,),
        out_shape=(
            jax.ShapeDtypeStruct((devices, 3 * CAP, width), F32),
            jax.ShapeDtypeStruct((3, local_count, node_count), F32),
        ),
        in_specs=[
            pl.BlockSpec((1, 1, batch), lambda i: (i, 0, 0)),
            pl.BlockSpec((batch, 9), lambda i: (i, 0)),
            pl.BlockSpec((groups, 6 * CAP, width), lambda i: (i, 0, 0)),
            vmem(),
            vmem(),
        ],
        out_specs=(
            pl.BlockSpec((groups, 3 * CAP, width), lambda i: (i, 0, 0)),
            pl.BlockSpec((3, local_count, node_count), lambda i: (0, 0, 0)),
        ),
        scratch_shapes=[
            pltpu.VMEM((batch, width), F32),
            pltpu.VMEM((width // 128, 32 * CAP, 128), F32),
            pltpu.VMEM((batch * width + spare, 128), F32),
            pltpu.VMEM((8, batch), jnp.int32),
            pltpu.VMEM((local_count, 128), jnp.int32),
            pltpu.SMEM((8, batch), jnp.int32),
            pltpu.SMEM((local_count, 128), jnp.int32),
            pltpu.VMEM((local_count, 8, node_count), F32),
            pltpu.SemaphoreType.DMA((2,)),
        ],
        compiler_params=pltpu.CompilerParams(vmem_limit_bytes=48 * 1024 * 1024),
        name="couple",
    )(asked.reshape(-1, 1, batch), boxes, arrived, node_rows, coeff_rows)

    back = lax.all_to_all(values, AXES, split_axis=0, concat_axis=0, tiled=True)
    point_disp = pl.pallas_call(
        unpack_kernel,
        out_shape=jax.ShapeDtypeStruct((3, tile_total, width), F32),
        in_specs=[smem(), vmem(), vmem()],
        out_specs=vmem(),
        name="unpack",
    )(slot_of, back, pu_level)
    return jnp.transpose(point_disp, (1, 0, 2)), jnp.transpose(node_force, (1, 0, 2))


def solution(mesh):
    placed = (
        P(AXES, None, None),
        P(AXES, None, None),
        P(AXES, None),
        P(AXES, None, None),
        P(AXES, None, None),
        P(AXES, None, None),
        P(AXES, None, None),
    )
    return jax.shard_map(
        on_device,
        mesh=mesh,
        in_specs=placed,
        out_specs=(P(AXES, None, None), P(AXES, None, None)),
        check_vma=False,
    )
```

```python
import functools

import jax
import jax.numpy as jnp
from jax import lax
from jax.experimental import pallas as pl
from jax.experimental.pallas import tpu as pltpu
from jax.sharding import PartitionSpec as P

CAP = 8
PARTS = 2
SHARE = CAP // PARTS
GROUP = 8
BATCH = 128
CHUNK = 256
WINDOW = 96
LANES = 128
AXES = ("row", "col")
NT = (((1,), (1,)), ((), ()))
F32 = jnp.float32
BF16 = jnp.bfloat16


def rounded(x):
    return x.astype(BF16).astype(F32)


def split2(x):
    high = rounded(x)
    return high, rounded(x - high)


def split3(x):
    high = rounded(x)
    rest = x - high
    middle = rounded(rest)
    return high, middle, rounded(rest - middle)


def outer_split(x, parts):
    pieces = []
    for _ in range(parts):
        piece = lax.reduce_precision(x, 8, 7)
        pieces.append(piece)
        x = x - piece
    return pieces


def tile_weights(levels):
    levels = levels.astype(F32) + 1.0
    return levels / jnp.sum(levels, axis=0, keepdims=True)


def iota(shape, axis):
    return lax.broadcasted_iota(jnp.int32, shape, axis)


def as_bf16(mask):
    return mask.astype(F32).astype(BF16)


def copy_slots(part, pair_of, points, loads, out):
    devices = out.shape[0]
    halves = points.shape[2] // LANES
    kslots = loads.shape[1] // points.shape[1]

    @pl.loop(0, devices)
    def _(d):
        for j in range(SHARE):
            pair = jnp.maximum(pair_of[d * CAP + part * SHARE + j], 0)
            tile = pair // kslots
            for c in range(6):
                whole = points[c, pl.ds(tile, 1), :] if c < 3 else loads[c - 3, pl.ds(pair, 1), :]
                for h in range(halves):
                    row = c * GROUP + h * SHARE + j
                    out[d, row : row + 1, :] = whole[:, h * LANES : (h + 1) * LANES]


def first_pack_kernel(local_count, full, ids, points, force, level, out, loads, pair_of, count):
    devices = out.shape[0]
    tiles, kslots = level.shape[0], level.shape[1]

    @pl.loop(0, devices)
    def _(d):
        count[d] = 0
        if not full:
            out[d, 6 * GROUP : 7 * GROUP, :] = jnp.full((CAP, LANES), -1.0, F32)
            for j in range(CAP):
                pair_of[d * CAP + j] = -1

    @pl.loop(0, tiles)
    def _(t):
        weights = tile_weights(level[t])
        for c in range(3):
            where = pl.ds(pl.multiple_of(t * kslots, kslots), kslots)
            loads[c, where, :] = weights * (force[c, pl.ds(t, 1), :] * (1.0 / 256.0))
        for k in range(kslots):
            pair = t * kslots + k
            cluster = ids[pair]
            d = cluster // local_count
            j = count[d]
            count[d] = j + 1
            pair_of[d * CAP + j] = pair
            own = (cluster - d * local_count).astype(F32)
            out[d, pl.ds(6 * GROUP + j, 1), :] = jnp.full((1, LANES), own)

    copy_slots(0, pair_of, points, loads, out)


def next_pack_kernel(part, pair_of, points, loads, out):
    copy_slots(part, pair_of, points, loads, out)


def unpack_kernel(pair_of, *refs):
    backs, level, out, rows = refs[:PARTS], refs[PARTS], refs[PARTS + 1], refs[PARTS + 2]
    tiles, kslots = level.shape[0], level.shape[1]
    halves = out.shape[2] // LANES
    devices = backs[0].shape[0]

    @pl.loop(0, devices)
    def _(d):
        for slot in range(CAP):
            pair = pair_of[d * CAP + slot]
            pair = jnp.where(pair < 0, tiles * kslots, pair)
            back, j = backs[slot // SHARE], slot % SHARE
            for c in range(3):
                pieces = [
                    back[d, c * GROUP + h * SHARE + j : c * GROUP + h * SHARE + j + 1, :]
                    for h in range(halves)
                ]
                rows[c, pl.ds(pair, 1), :] = jnp.concatenate(pieces, axis=1)

    @pl.loop(0, tiles)
    def _(t):
        weights = tile_weights(level[t])
        where = pl.ds(pl.multiple_of(t * kslots, kslots), kslots)
        for c in range(3):
            out[c, pl.ds(t, 1), :] = jnp.sum(weights * rows[c, where, :], axis=0, keepdims=True)


def couple_kernel(part, *refs):
    refs = list(refs)
    first, last = part == 0, part == PARTS - 1
    id_tiles, arrived, table, node_rows, coeff_rows = refs[:5]
    del refs[:5]
    earlier_force = None if first else refs.pop(0)
    values, node_force = refs[:2]
    (
        rank,
        id_rows,
        boxes,
        rows,
        packed,
        even,
        odd,
        slot_plan_v,
        cluster_plan_v,
        slot_plan,
        cluster_plan,
        cluster_of,
        force_sum,
        sems,
    ) = refs[2:]
    sources = arrived.shape[0]
    batch = sources * SHARE
    groups = batch // GROUP
    per_group = GROUP // SHARE
    halves = GROUP // SHARE
    width = halves * LANES
    clusters = node_rows.shape[0]
    step = pl.program_id(0)

    @pl.when(step == 0)
    def _():
        if first:
            force_sum[...] = jnp.zeros_like(force_sum)
        else:
            force_sum[...] = earlier_force[...]

    def group_rows(g):
        return pl.ds(pl.multiple_of(g * GROUP, GROUP), GROUP)

    @pl.loop(0, groups)
    def _(g):
        id_rows[group_rows(g), :] = jnp.concatenate(
            [
                id_tiles[g * per_group + i, part * SHARE : (part + 1) * SHARE, :]
                for i in range(per_group)
            ],
            axis=0,
        )

    lane = iota((1, LANES), 1)
    own = id_rows[...]
    thrice = (own == (lane % clusters).astype(F32)) & (lane < 3 * clusters)
    boxes[...] = jnp.dot(as_bf16(thrice), table[...], preferred_element_type=F32)

    def slot_tiles(box, i):
        return jnp.concatenate([box[i * SHARE : (i + 1) * SHARE]] * halves, axis=0)

    @pl.loop(0, groups)
    def _(g):
        found = []
        for i in range(per_group):
            d = g * per_group + i
            box = slot_tiles(boxes[group_rows(g), :], i)
            gap = jnp.where(slot_tiles(id_rows[group_rows(g), :], i) < 0.0, 4.0, 0.0)
            for c in range(3):
                x = arrived[d, c * GROUP : (c + 1) * GROUP, :]
                side = jnp.maximum(box[:, c : c + 1] - x, x - box[:, 3 + c : 4 + c])
                side = jnp.maximum(side, 0.0)
                gap = gap + side * side
            found.append(jnp.where(gap < 1.0002, 1.0, 0.0))
        for h in range(halves):
            rank[group_rows(g), h * LANES : (h + 1) * LANES] = jnp.concatenate(
                [tile[h * SHARE : (h + 1) * SHARE] for tile in found], axis=0
            )

    near = rank[...].astype(BF16)
    before = as_bf16(iota((width, width), 0) < iota((width, width), 1))
    earlier = jnp.dot(near, before, preferred_element_type=F32)
    rank[...] = jnp.where(near.astype(F32) > 0.5, earlier, -1e6)
    counts = lax.dot_general(jnp.ones((8, width), BF16), near, NT, preferred_element_type=F32)
    pick = as_bf16(iota((clusters, LANES), 0) == iota((clusters, LANES), 1))
    hits = lax.dot_general(
        pick, as_bf16(own == lane.astype(F32)), NT, preferred_element_type=F32
    )
    hit_counts = hits * counts[0:1]
    before_slot = as_bf16(iota((batch, batch), 0) < iota((batch, batch), 1))
    slot_start = jnp.dot(hit_counts.astype(BF16), before_slot, preferred_element_type=F32)
    totals = jnp.sum(hit_counts, axis=1, keepdims=True)
    chunks = jnp.floor((totals + (CHUNK - 1)) * (1.0 / CHUNK))
    chunks = jnp.broadcast_to(chunks, (clusters, LANES))
    before_cluster = as_bf16(iota((clusters, clusters), 1) < iota((clusters, clusters), 0))
    first_chunk = jnp.dot(before_cluster, chunks.astype(BF16), preferred_element_type=F32)
    offset = jnp.sum(hits * (slot_start + first_chunk[:, 0:1] * CHUNK), axis=0, keepdims=True)
    slot_plan_v[0:1, :] = offset.astype(jnp.int32)
    slot_plan_v[1:2, :] = counts[0:1].astype(jnp.int32)
    cluster_plan_v[...] = jnp.where(lane == 0, first_chunk, chunks).astype(jnp.int32)
    copies = [
        pltpu.make_async_copy(slot_plan_v, slot_plan, sems.at[0]),
        pltpu.make_async_copy(cluster_plan_v, cluster_plan, sems.at[1]),
    ]
    for copy in copies:
        copy.start()
    for copy in copies:
        copy.wait()
    total_chunks = cluster_plan[clusters - 1, 0] + cluster_plan[clusters - 1, 1]

    @pl.loop(0, clusters)
    def _(c):
        @pl.loop(0, cluster_plan[c, 1])
        def _(j):
            cluster_of[cluster_plan[c, 0] + j] = c

    def chunk_rows(j):
        return pl.ds(pl.multiple_of(j * CHUNK, CHUNK), CHUNK)

    @pl.loop(0, total_chunks + 3)
    def _(j):
        packed[chunk_rows(j), :] = jnp.zeros((CHUNK, LANES), F32)

    for extra in range(3):
        cluster_of[total_chunks + extra] = 0

    target = iota((WINDOW, 1), 0).astype(F32)

    def places_of(g):
        places = []
        for i in range(GROUP):
            slot = g * GROUP + i
            start = slot_plan[0, slot]
            base = (start // 8) * 8
            lead = start - base
            blocks = (lead + slot_plan[1, slot] + (WINDOW - 1)) // WINDOW
            places.append((rank[pl.ds(slot, 1), :], base, lead, blocks))
        most = places[0][3]
        for place in places[1:]:
            most = jnp.maximum(most, place[3])
        return places, most

    def selection(place, block):
        shift = (place[2] - block * WINDOW).astype(F32)
        return jnp.where(place[0] + shift == target, 1.0, 0.0).astype(BF16)

    def window_of(place, block):
        return pl.ds(pl.multiple_of(place[1] + block * WINDOW, 8), WINDOW)

    @pl.loop(0, groups)
    def _(g):
        for i in range(per_group):
            d = g * per_group + i
            box = slot_tiles(boxes[group_rows(g), :], i)
            x = [
                arrived[d, c * GROUP : (c + 1) * GROUP, :] - box[:, 6 + c : 7 + c] for c in range(3)
            ]
            parts = [split3(v) for v in x]
            square = split3(x[0] * x[0] + x[1] * x[1] + x[2] * x[2])
            loads = [split2(arrived[d, (3 + c) * GROUP : (4 + c) * GROUP, :]) for c in range(3)]
            column = [parts[c][p] for p in (0, 1, 2, 0, 1, 0) for c in range(3)]
            column += list(square) + [jnp.ones_like(x[0])] * 3
            column += [loads[c][p] for p in range(2) for c in range(3)]
            column += [jnp.zeros_like(x[0])] * 2
            for n, tile in enumerate(column):
                rows[i, n * GROUP : (n + 1) * GROUP, :] = tile
        places, most = places_of(g)

        def gathered(i, block):
            source = rows.at[i // SHARE]
            pieces = [
                source[pl.ds(h * SHARE + i % SHARE, 32, stride=GROUP), :] for h in range(halves)
            ]
            return lax.dot_general(
                selection(places[i], block),
                jnp.concatenate(pieces, axis=1).astype(BF16),
                NT,
                preferred_element_type=F32,
            )

        moved = [gathered(i, 0) for i in range(GROUP)]
        for i in range(GROUP):
            packed[window_of(places[i], 0), 0:32] += moved[i]

        @pl.when(most > 1)
        def _():
            for i in range(GROUP):

                @pl.loop(1, places[i][3])
                def _(block):
                    packed[window_of(places[i], block), 0:32] += gathered(i, block)

    def distances(j, squares):
        squares[...] = jnp.dot(
            packed[chunk_rows(j), 0:32].astype(BF16),
            node_rows[cluster_of[j]],
            preferred_element_type=F32,
        )

    def contract(j, squares):
        c = cluster_of[j]
        square = jnp.maximum(squares[...], 1e-30)
        rest = jnp.maximum(4.0 - square * lax.rsqrt(square), 0.0)
        rest2 = rest * rest
        kernel = (rest2 * rest2) * (5.0 - rest)
        high = kernel.astype(BF16)
        low = (kernel - high.astype(F32)).astype(BF16)
        loads = jnp.transpose(packed[chunk_rows(j), :])[24:32].astype(BF16)
        packed[chunk_rows(j), 0:16] = lax.dot_general(
            high, coeff_rows[c], NT, preferred_element_type=F32
        ) + lax.dot_general(low, coeff_rows[c], NT, preferred_element_type=F32)
        force_sum[c] += jnp.dot(loads, high, preferred_element_type=F32) + jnp.dot(
            loads, low, preferred_element_type=F32
        )

    distances(0, even)

    @pl.loop(0, (total_chunks + 1) // 2)
    def _(j):
        distances(2 * j + 1, odd)
        contract(2 * j, even)
        distances(2 * j + 2, even)
        contract(2 * j + 1, odd)

    @pl.loop(0, groups)
    def _(g):
        places, most = places_of(g)

        def spread(i, block):
            rows_t = jnp.transpose(packed[window_of(places[i], block), :])
            high, middle, low = split3(rows_t[0:8] + rows_t[8:16])
            stacked = jnp.concatenate([high, middle, low], axis=0).astype(BF16)
            moved = jnp.dot(stacked, selection(places[i], block), preferred_element_type=F32)
            return moved[0:8] + moved[8:16] + moved[16:24]

        def pieces_of(i, found):
            d = g * per_group + i // SHARE
            for c in range(3):
                for h in range(halves):
                    row = c * GROUP + h * SHARE + i % SHARE
                    yield d, row, found[c : c + 1, h * LANES : (h + 1) * LANES]

        spreads = [spread(i, 0) for i in range(GROUP)]
        for i in range(GROUP):
            for d, row, piece in pieces_of(i, spreads[i]):
                values[d, row : row + 1, :] = piece

        @pl.when(most > 1)
        def _():
            for i in range(GROUP):

                @pl.loop(1, places[i][3])
                def _(block):
                    for d, row, piece in pieces_of(i, spread(i, block)):
                        values[d, row : row + 1, :] += piece

    @pl.when(step == pl.num_programs(0) - 1)
    def _():
        if last:
            for c in range(clusters):
                both = force_sum[c]
                for i in range(3):
                    node_force[i, c : c + 1, :] = both[i : i + 1] + both[3 + i : 4 + i]
        else:
            node_force[...] = force_sum[...]


def vmem():
    return pl.BlockSpec(memory_space=pltpu.VMEM)


def smem():
    return pl.BlockSpec(memory_space=pltpu.SMEM)


def couple(part, id_source, arrived, table, node_rows, coeff_rows, earlier_force):
    devices = arrived.shape[0]
    clusters, _, nodes = node_rows.shape
    batch = min(BATCH, devices * SHARE)
    sources = batch // SHARE
    width = GROUP // SHARE * LANES
    last = part == PARTS - 1
    force_shape = (3, clusters, nodes) if last else (clusters, 8, nodes)
    room = batch * width + clusters * CHUNK + 3 * CHUNK + 2 * WINDOW
    extra = () if earlier_force is None else (earlier_force,)
    pairs = devices * SHARE * width // 4
    return pl.pallas_call(
        functools.partial(couple_kernel, part),
        grid=(devices * SHARE // batch,),
        out_shape=(
            jax.ShapeDtypeStruct((devices, 3 * GROUP, LANES), F32),
            jax.ShapeDtypeStruct(force_shape, F32),
        ),
        in_specs=[
            pl.BlockSpec((sources, GROUP, LANES), lambda i: (i, 6, 0)),
            pl.BlockSpec((sources, 6 * GROUP, LANES), lambda i: (i, 0, 0)),
            vmem(),
            vmem(),
            vmem(),
        ]
        + [vmem() for _ in extra],
        out_specs=(
            pl.BlockSpec((sources, 3 * GROUP, LANES), lambda i: (i, 0, 0)),
            pl.BlockSpec(force_shape, lambda i: (0, 0, 0)),
        ),
        scratch_shapes=[
            pltpu.VMEM((batch, width), F32),
            pltpu.VMEM((batch, LANES), F32),
            pltpu.VMEM((batch, LANES), F32),
            pltpu.VMEM((GROUP // SHARE, 32 * GROUP, LANES), F32),
            pltpu.VMEM((room, LANES), F32),
            pltpu.VMEM((CHUNK, nodes), F32),
            pltpu.VMEM((CHUNK, nodes), F32),
            pltpu.VMEM((8, batch), jnp.int32),
            pltpu.VMEM((clusters, LANES), jnp.int32),
            pltpu.SMEM((8, batch), jnp.int32),
            pltpu.SMEM((clusters, LANES), jnp.int32),
            pltpu.SMEM((room // CHUNK + 4,), jnp.int32),
            pltpu.VMEM((clusters, 8, nodes), F32),
            pltpu.SemaphoreType.DMA((2,)),
        ],
        compiler_params=pltpu.CompilerParams(vmem_limit_bytes=40 * 1024 * 1024),
        cost_estimate=pl.CostEstimate(
            flops=pairs * nodes * 80, bytes_accessed=arrived.size * 6, transcendentals=pairs * nodes
        ),
        name=f"couple_{part}",
    )(id_source, arrived, table, node_rows, coeff_rows, *extra)


def exchange(x):
    return lax.all_to_all(x, AXES, split_axis=0, concat_axis=0, tiled=True)


def on_device(point_coords, fluid_force, tile_clusters, pu_level, node_coords, node_disp, inverse):
    highest = lax.Precision.HIGHEST
    devices = lax.axis_size(AXES)
    slot_total = devices * CAP
    tile_total, kslots = tile_clusters.shape
    pair_total = tile_total * kslots
    local_count, _, node_count = node_coords.shape
    width = point_coords.shape[2]
    points = jnp.transpose(point_coords, (1, 0, 2))

    outgoing, loads, pair_of = pl.pallas_call(
        functools.partial(first_pack_kernel, local_count, pair_total == slot_total),
        out_shape=(
            jax.ShapeDtypeStruct((devices, 7 * GROUP, LANES), F32),
            jax.ShapeDtypeStruct((3, pair_total, width), F32),
            jax.ShapeDtypeStruct((slot_total,), jnp.int32),
        ),
        in_specs=[smem(), vmem(), vmem(), vmem()],
        out_specs=(vmem(), vmem(), smem()),
        scratch_shapes=[pltpu.SMEM((devices,), jnp.int32)],
        name="pack_0",
    )(tile_clusters.reshape(-1), points, jnp.transpose(fluid_force, (1, 0, 2)), pu_level)
    arrived = exchange(outgoing)

    coeffs = jnp.einsum("cin,cnm->cim", node_disp, inverse, precision=highest) * (1.0 / 256.0)
    high, low = outer_split(coeffs, 2)
    gap5 = jnp.zeros((local_count, 5, node_count), F32)
    coeff_rows = jnp.concatenate((high, gap5, low, gap5), axis=1).astype(BF16)
    least = jnp.min(node_coords, axis=2)
    most = jnp.max(node_coords, axis=2)
    centre = 0.5 * (least + most)
    nodes = node_coords - centre[:, :, None]
    near = [-32.0 * piece for piece in outer_split(nodes, 3)]
    square = [16.0 * p for p in outer_split(jnp.sum(nodes * nodes, axis=1, keepdims=True), 3)]
    sixteen = jnp.full((local_count, 3, node_count), 16.0, F32)
    rows = [near[0]] * 3 + [near[1]] * 2 + [near[2], sixteen] + square
    rows.append(jnp.zeros((local_count, 8, node_count), F32))
    node_rows = jnp.concatenate(rows, axis=1).astype(BF16)
    table = jnp.concatenate((least, most, centre), axis=1)
    table = jnp.concatenate(outer_split(table, 3), axis=0).astype(BF16)
    table = jnp.pad(table, ((0, LANES - table.shape[0]), (0, LANES - table.shape[1])))

    id_source = arrived
    force = None
    backs = []
    for part in range(PARTS):
        following = None
        if part + 1 < PARTS:
            packed = pl.pallas_call(
                functools.partial(next_pack_kernel, part + 1),
                out_shape=jax.ShapeDtypeStruct((devices, 6 * GROUP, LANES), F32),
                in_specs=[smem(), vmem(), vmem()],
                out_specs=vmem(),
                name=f"pack_{part + 1}",
            )(pair_of, points, loads)
            packed, arrived, table, node_rows, coeff_rows = lax.optimization_barrier(
                (packed, arrived, table, node_rows, coeff_rows)
            )
            if part == 0:
                id_source = arrived
            following = exchange(packed)
        values, force = couple(part, id_source, arrived, table, node_rows, coeff_rows, force)
        backs.append(exchange(values))
        arrived = following

    point_disp = pl.pallas_call(
        unpack_kernel,
        out_shape=jax.ShapeDtypeStruct((3, tile_total, width), F32),
        in_specs=[smem()] + [vmem()] * (PARTS + 1),
        out_specs=vmem(),
        scratch_shapes=[pltpu.VMEM((3, pair_total + 8, width), F32)],
        name="unpack",
    )(pair_of, *backs, pu_level)
    return jnp.transpose(point_disp, (1, 0, 2)), jnp.transpose(force, (1, 0, 2))


def solution(mesh):
    placed = (
        P(AXES, None, None),
        P(AXES, None, None),
        P(AXES, None),
        P(AXES, None, None),
        P(AXES, None, None),
        P(AXES, None, None),
        P(AXES, None, None),
    )
    return jax.shard_map(
        on_device,
        mesh=mesh,
        in_specs=placed,
        out_specs=(P(AXES, None, None), P(AXES, None, None)),
        check_vma=False,
    )
```

```python
import functools

import jax
import jax.numpy as jnp
from jax import lax
from jax.experimental import pallas as pl
from jax.experimental.pallas import tpu as pltpu
from jax.sharding import PartitionSpec as P

CAP = 8
PARTS = 2
SHARE = CAP // PARTS
GROUP = 8
BATCH = 128
CHUNK = 256
TEAM = 4
WINDOW = 96
LANES = 128
AXES = ("row", "col")
NT = (((1,), (1,)), ((), ()))
F32 = jnp.float32
BF16 = jnp.bfloat16


def rounded(x):
    return x.astype(BF16).astype(F32)


def split2(x):
    high = rounded(x)
    return high, rounded(x - high)


def split3(x):
    high = rounded(x)
    rest = x - high
    middle = rounded(rest)
    return high, middle, rounded(rest - middle)


def outer_split(x, parts):
    pieces = []
    for _ in range(parts):
        piece = lax.reduce_precision(x, 8, 7)
        pieces.append(piece)
        x = x - piece
    return pieces


def tile_weights(levels):
    levels = levels.astype(F32) + 1.0
    return levels / jnp.sum(levels, axis=0, keepdims=True)


def iota(shape, axis):
    return lax.broadcasted_iota(jnp.int32, shape, axis)


def as_bf16(mask):
    return mask.astype(F32).astype(BF16)


def copy_slots(part, pair_of, points, loads, out):
    devices = out.shape[0]
    halves = points.shape[2] // LANES
    kslots = loads.shape[1] // points.shape[1]

    @pl.loop(0, devices)
    def _(d):
        for j in range(SHARE):
            pair = jnp.maximum(pair_of[d * CAP + part * SHARE + j], 0)
            tile = pair // kslots
            for c in range(6):
                whole = points[c, pl.ds(tile, 1), :] if c < 3 else loads[c - 3, pl.ds(pair, 1), :]
                for h in range(halves):
                    row = c * GROUP + h * SHARE + j
                    out[d, row : row + 1, :] = whole[:, h * LANES : (h + 1) * LANES]


def first_pack_kernel(local_count, full, ids, points, force, level, out, loads, pair_of, count):
    devices = out.shape[0]
    tiles, kslots = level.shape[0], level.shape[1]

    @pl.loop(0, devices)
    def _(d):
        count[d] = 0
        if not full:
            out[d, 6 * GROUP : 7 * GROUP, :] = jnp.full((CAP, LANES), -1.0, F32)
            for j in range(CAP):
                pair_of[d * CAP + j] = -1

    @pl.loop(0, tiles)
    def _(t):
        weights = tile_weights(level[t])
        for c in range(3):
            where = pl.ds(pl.multiple_of(t * kslots, kslots), kslots)
            loads[c, where, :] = weights * (force[c, pl.ds(t, 1), :] * (1.0 / 256.0))
        for k in range(kslots):
            pair = t * kslots + k
            cluster = ids[pair]
            d = cluster // local_count
            j = count[d]
            count[d] = j + 1
            pair_of[d * CAP + j] = pair
            own = (cluster - d * local_count).astype(F32)
            out[d, pl.ds(6 * GROUP + j, 1), :] = jnp.full((1, LANES), own)

    copy_slots(0, pair_of, points, loads, out)


def next_pack_kernel(part, pair_of, points, loads, out):
    copy_slots(part, pair_of, points, loads, out)


def unpack_kernel(pair_of, *refs):
    backs, level, out, rows = refs[:PARTS], refs[PARTS], refs[PARTS + 1], refs[PARTS + 2]
    tiles, kslots = level.shape[0], level.shape[1]
    halves = out.shape[2] // LANES
    devices = backs[0].shape[0]

    @pl.loop(0, devices)
    def _(d):
        for slot in range(CAP):
            pair = pair_of[d * CAP + slot]
            pair = jnp.where(pair < 0, tiles * kslots, pair)
            back, j = backs[slot // SHARE], slot % SHARE
            for c in range(3):
                pieces = [
                    back[d, c * GROUP + h * SHARE + j : c * GROUP + h * SHARE + j + 1, :]
                    for h in range(halves)
                ]
                rows[c, pl.ds(pair, 1), :] = jnp.concatenate(pieces, axis=1)

    @pl.loop(0, tiles)
    def _(t):
        weights = tile_weights(level[t])
        where = pl.ds(pl.multiple_of(t * kslots, kslots), kslots)
        for c in range(3):
            out[c, pl.ds(t, 1), :] = jnp.sum(weights * rows[c, where, :], axis=0, keepdims=True)


def couple_kernel(part, *refs):
    refs = list(refs)
    first, last = part == 0, part == PARTS - 1
    id_tiles, arrived, table, node_rows, coeff_rows = refs[:5]
    del refs[:5]
    earlier_force = None if first else refs.pop(0)
    id_row = id_tiles.shape[1] - CAP + part * SHARE
    values, node_force = refs[:2]
    (
        rank,
        id_rows,
        boxes,
        rows,
        packed,
        found_rows,
        even,
        odd,
        slot_plan_v,
        cluster_plan_v,
        slot_plan,
        cluster_plan,
        cluster_of,
        force_sum,
        sems,
    ) = refs[2:]
    sources = arrived.shape[0]
    batch = sources * SHARE
    groups = batch // GROUP
    per_group = GROUP // SHARE
    halves = GROUP // SHARE
    width = halves * LANES
    clusters = node_rows.shape[0]
    step = pl.program_id(0)

    @pl.when(step == 0)
    def _():
        if first:
            force_sum[...] = jnp.zeros_like(force_sum)
        else:
            force_sum[...] = earlier_force[...]

    def group_rows(g):
        return pl.ds(pl.multiple_of(g * GROUP, GROUP), GROUP)

    @pl.loop(0, groups)
    def _(g):
        id_rows[group_rows(g), :] = jnp.concatenate(
            [
                id_tiles[g * per_group + i, id_row : id_row + SHARE, :]
                for i in range(per_group)
            ],
            axis=0,
        )

    lane = iota((1, LANES), 1)
    own = id_rows[...]
    thrice = (own == (lane % clusters).astype(F32)) & (lane < 3 * clusters)
    boxes[...] = jnp.dot(as_bf16(thrice), table[...], preferred_element_type=F32)

    def slot_tiles(box, i):
        return jnp.concatenate([box[i * SHARE : (i + 1) * SHARE]] * halves, axis=0)

    @pl.loop(0, groups)
    def _(g):
        found = []
        for i in range(per_group):
            d = g * per_group + i
            box = slot_tiles(boxes[group_rows(g), :], i)
            gap = jnp.where(slot_tiles(id_rows[group_rows(g), :], i) < 0.0, 4.0, 0.0)
            for c in range(3):
                x = arrived[d, c * GROUP : (c + 1) * GROUP, :]
                side = jnp.maximum(box[:, c : c + 1] - x, x - box[:, 3 + c : 4 + c])
                side = jnp.maximum(side, 0.0)
                gap = gap + side * side
            found.append(jnp.where(gap < 1.0002, 1.0, 0.0))
        for h in range(halves):
            rank[group_rows(g), h * LANES : (h + 1) * LANES] = jnp.concatenate(
                [tile[h * SHARE : (h + 1) * SHARE] for tile in found], axis=0
            )

    near = rank[...].astype(BF16)
    before = as_bf16(iota((width, width), 0) < iota((width, width), 1))
    earlier = jnp.dot(near, before, preferred_element_type=F32)
    rank[...] = jnp.where(near.astype(F32) > 0.5, earlier, -1e6)
    counts = lax.dot_general(jnp.ones((8, width), BF16), near, NT, preferred_element_type=F32)
    pick = as_bf16(iota((clusters, LANES), 0) == iota((clusters, LANES), 1))
    hits = lax.dot_general(
        pick, as_bf16(own == lane.astype(F32)), NT, preferred_element_type=F32
    )
    hit_counts = hits * counts[0:1]
    before_slot = as_bf16(iota((batch, batch), 0) < iota((batch, batch), 1))
    slot_start = jnp.dot(hit_counts.astype(BF16), before_slot, preferred_element_type=F32)
    totals = jnp.sum(hit_counts, axis=1, keepdims=True)
    chunks = jnp.floor((totals + (CHUNK - 1)) * (1.0 / CHUNK))
    chunks = jnp.broadcast_to(chunks, (clusters, LANES))
    before_cluster = as_bf16(iota((clusters, clusters), 1) < iota((clusters, clusters), 0))
    first_chunk = jnp.dot(before_cluster, chunks.astype(BF16), preferred_element_type=F32)
    offset = jnp.sum(hits * (slot_start + first_chunk[:, 0:1] * CHUNK), axis=0, keepdims=True)
    slot_plan_v[0:1, :] = offset.astype(jnp.int32)
    slot_plan_v[1:2, :] = counts[0:1].astype(jnp.int32)
    cluster_plan_v[...] = jnp.where(lane == 0, first_chunk, chunks).astype(jnp.int32)
    copies = [
        pltpu.make_async_copy(slot_plan_v, slot_plan, sems.at[0]),
        pltpu.make_async_copy(cluster_plan_v, cluster_plan, sems.at[1]),
    ]
    for copy in copies:
        copy.start()
    for copy in copies:
        copy.wait()
    total_chunks = cluster_plan[clusters - 1, 0] + cluster_plan[clusters - 1, 1]

    @pl.loop(0, clusters)
    def _(c):
        @pl.loop(0, cluster_plan[c, 1])
        def _(j):
            cluster_of[cluster_plan[c, 0] + j] = c

    def chunk_rows(j):
        return pl.ds(pl.multiple_of(j * CHUNK, CHUNK), CHUNK)

    @pl.loop(0, total_chunks + 3)
    def _(j):
        packed[chunk_rows(j), :] = jnp.zeros((CHUNK, LANES), F32)

    for extra in range(2):
        found_rows[chunk_rows(total_chunks + extra), 0:16] = jnp.zeros((CHUNK, 16), F32)

    for extra in range(3):
        cluster_of[total_chunks + extra] = 0

    target = iota((WINDOW, 1), 0).astype(F32)

    def places_of(team):
        places = []
        for i in range(TEAM * GROUP):
            slot = team * (TEAM * GROUP) + i
            start = slot_plan[0, slot]
            base = (start // 8) * 8
            lead = start - base
            blocks = (lead + slot_plan[1, slot] + (WINDOW - 1)) // WINDOW
            places.append((rank[pl.ds(slot, 1), :], base, lead, blocks))
        most = places[0][3]
        for place in places[1:]:
            most = jnp.maximum(most, place[3])
        return places, most

    def selection(place, block):
        shift = (place[2] - block * WINDOW).astype(F32)
        return jnp.where(place[0] + shift == target, 1.0, 0.0).astype(BF16)

    def window_of(place, block):
        return pl.ds(pl.multiple_of(place[1] + block * WINDOW, 8), WINDOW)

    @pl.loop(0, groups // TEAM)
    def _(team):
        for i in range(TEAM * per_group):
            d = team * (TEAM * per_group) + i
            box = slot_tiles(boxes[group_rows(team * TEAM + i // per_group), :], i % per_group)
            x = [
                arrived[d, c * GROUP : (c + 1) * GROUP, :] - box[:, 6 + c : 7 + c] for c in range(3)
            ]
            parts = [split3(v) for v in x]
            square = split3(x[0] * x[0] + x[1] * x[1] + x[2] * x[2])
            loads = [split2(arrived[d, (3 + c) * GROUP : (4 + c) * GROUP, :]) for c in range(3)]
            column = [parts[c][p] for p in (0, 1, 2, 0, 1, 0) for c in range(3)]
            column += list(square) + [jnp.ones_like(x[0])] * 3
            column += [loads[c][p] for p in range(2) for c in range(3)]
            column += [jnp.zeros_like(x[0])] * 2
            for n, tile in enumerate(column):
                rows[i, n * GROUP : (n + 1) * GROUP, :] = tile
        places, most = places_of(team)

        def gathered(i, block):
            source = rows.at[i // SHARE]
            pieces = [
                source[pl.ds(h * SHARE + i % SHARE, 32, stride=GROUP), :] for h in range(halves)
            ]
            return lax.dot_general(
                selection(places[i], block),
                jnp.concatenate(pieces, axis=1).astype(BF16),
                NT,
                preferred_element_type=F32,
            )

        moved = [gathered(i, 0) for i in range(TEAM * GROUP)]
        for i in range(TEAM * GROUP):
            packed[window_of(places[i], 0), 0:32] += moved[i]

        @pl.when(most > 1)
        def _():
            for i in range(TEAM * GROUP):

                @pl.loop(1, places[i][3])
                def _(block):
                    packed[window_of(places[i], block), 0:32] += gathered(i, block)

    def distances(j, squares):
        squares[...] = jnp.dot(
            packed[chunk_rows(j), 0:32].astype(BF16),
            node_rows[cluster_of[j]],
            preferred_element_type=F32,
        )

    def contract(j, squares):
        c = cluster_of[j]
        square = jnp.maximum(squares[...], 1e-30)
        rest = jnp.maximum(4.0 - square * lax.rsqrt(square), 0.0)
        rest2 = rest * rest
        kernel = (rest2 * rest2) * (5.0 - rest)
        high = kernel.astype(BF16)
        low = (kernel - high.astype(F32)).astype(BF16)
        loads = jnp.transpose(packed[chunk_rows(j), :])[24:32].astype(BF16)
        found_rows[chunk_rows(j), 0:16] = lax.dot_general(
            high, coeff_rows[c], NT, preferred_element_type=F32
        ) + lax.dot_general(low, coeff_rows[c], NT, preferred_element_type=F32)
        force_sum[c] += jnp.dot(loads, high, preferred_element_type=F32) + jnp.dot(
            loads, low, preferred_element_type=F32
        )

    distances(0, even)

    @pl.loop(0, (total_chunks + 1) // 2)
    def _(j):
        distances(2 * j + 1, odd)
        contract(2 * j, even)
        distances(2 * j + 2, even)
        contract(2 * j + 1, odd)

    @pl.loop(0, groups // TEAM)
    def _(team):
        places, most = places_of(team)

        def spread(i, block):
            rows_t = jnp.transpose(found_rows[window_of(places[i], block), :])
            high, middle, low = split3(rows_t[0:8] + rows_t[8:16])
            stacked = jnp.concatenate([high, middle, low], axis=0).astype(BF16)
            moved = jnp.dot(stacked, selection(places[i], block), preferred_element_type=F32)
            return moved[0:8] + moved[8:16] + moved[16:24]

        def pieces_of(i, found):
            d = team * (TEAM * per_group) + i // SHARE
            for c in range(3):
                for h in range(halves):
                    row = c * GROUP + h * SHARE + i % SHARE
                    yield d, row, found[c : c + 1, h * LANES : (h + 1) * LANES]

        spreads = [spread(i, 0) for i in range(TEAM * GROUP)]
        for i in range(TEAM * GROUP):
            for d, row, piece in pieces_of(i, spreads[i]):
                values[d, row : row + 1, :] = piece

        @pl.when(most > 1)
        def _():
            for i in range(TEAM * GROUP):

                @pl.loop(1, places[i][3])
                def _(block):
                    for d, row, piece in pieces_of(i, spread(i, block)):
                        values[d, row : row + 1, :] += piece

    @pl.when(step == pl.num_programs(0) - 1)
    def _():
        if last:
            for c in range(clusters):
                both = force_sum[c]
                for i in range(3):
                    node_force[i, c : c + 1, :] = both[i : i + 1] + both[3 + i : 4 + i]
        else:
            node_force[...] = force_sum[...]


def vmem():
    return pl.BlockSpec(memory_space=pltpu.VMEM)


def smem():
    return pl.BlockSpec(memory_space=pltpu.SMEM)


def couple(part, id_source, arrived, table, node_rows, coeff_rows, earlier_force):
    devices = arrived.shape[0]
    clusters, _, nodes = node_rows.shape
    batch = min(BATCH, devices * SHARE)
    sources = batch // SHARE
    width = GROUP // SHARE * LANES
    last = part == PARTS - 1
    steps = devices * SHARE // batch
    force_shape = (3, clusters, nodes) if last else (clusters, 8, nodes)
    room = batch * width + clusters * CHUNK + 3 * CHUNK + 2 * WINDOW
    extra = () if earlier_force is None else (earlier_force,)
    pairs = devices * SHARE * width // 4
    return pl.pallas_call(
        functools.partial(couple_kernel, part),
        grid=(steps,),
        out_shape=(
            jax.ShapeDtypeStruct((devices, 3 * GROUP, LANES), F32),
            jax.ShapeDtypeStruct(force_shape, F32),
        ),
        in_specs=[
            vmem() if steps == 1 else pl.BlockSpec((sources, GROUP, LANES), lambda i: (i, 6, 0)),
            vmem() if steps == 1 else pl.BlockSpec((sources, 6 * GROUP, LANES), lambda i: (i, 0, 0)),
            vmem(),
            vmem(),
            vmem(),
        ]
        + [vmem() for _ in extra],
        out_specs=(
            vmem() if steps == 1 else pl.BlockSpec((sources, 3 * GROUP, LANES), lambda i: (i, 0, 0)),
            vmem() if steps == 1 else pl.BlockSpec(force_shape, lambda i: (0, 0, 0)),
        ),
        scratch_shapes=[
            pltpu.VMEM((batch, width), F32),
            pltpu.VMEM((batch, LANES), F32),
            pltpu.VMEM((batch, LANES), F32),
            pltpu.VMEM((TEAM * GROUP // SHARE, 32 * GROUP, LANES), F32),
            pltpu.VMEM((room, LANES), F32),
            pltpu.VMEM((room, LANES), F32),
            pltpu.VMEM((CHUNK, nodes), F32),
            pltpu.VMEM((CHUNK, nodes), F32),
            pltpu.VMEM((8, batch), jnp.int32),
            pltpu.VMEM((clusters, LANES), jnp.int32),
            pltpu.SMEM((8, batch), jnp.int32),
            pltpu.SMEM((clusters, LANES), jnp.int32),
            pltpu.SMEM((room // CHUNK + 4,), jnp.int32),
            pltpu.VMEM((clusters, 8, nodes), F32),
            pltpu.SemaphoreType.DMA((2,)),
        ],
        compiler_params=pltpu.CompilerParams(vmem_limit_bytes=52 * 1024 * 1024),
        cost_estimate=pl.CostEstimate(
            flops=pairs * nodes * 80, bytes_accessed=arrived.size * 6, transcendentals=pairs * nodes
        ),
        name=f"couple_{part}",
    )(id_source, arrived, table, node_rows, coeff_rows, *extra)


def exchange(x):
    return lax.all_to_all(x, AXES, split_axis=0, concat_axis=0, tiled=True)


def on_device(point_coords, fluid_force, tile_clusters, pu_level, node_coords, node_disp, inverse):
    highest = lax.Precision.HIGHEST
    devices = lax.axis_size(AXES)
    slot_total = devices * CAP
    tile_total, kslots = tile_clusters.shape
    pair_total = tile_total * kslots
    local_count, _, node_count = node_coords.shape
    width = point_coords.shape[2]
    points = jnp.transpose(point_coords, (1, 0, 2))

    outgoing, loads, pair_of = pl.pallas_call(
        functools.partial(first_pack_kernel, local_count, pair_total == slot_total),
        out_shape=(
            jax.ShapeDtypeStruct((devices, 7 * GROUP, LANES), F32),
            jax.ShapeDtypeStruct((3, pair_total, width), F32),
            jax.ShapeDtypeStruct((slot_total,), jnp.int32),
        ),
        in_specs=[smem(), vmem(), vmem(), vmem()],
        out_specs=(vmem(), vmem(), smem()),
        scratch_shapes=[pltpu.SMEM((devices,), jnp.int32)],
        name="pack_0",
    )(tile_clusters.reshape(-1), points, jnp.transpose(fluid_force, (1, 0, 2)), pu_level)
    arrived = exchange(outgoing)

    coeffs = jnp.einsum("cin,cnm->cim", node_disp, inverse, precision=highest) * (1.0 / 256.0)
    high, low = outer_split(coeffs, 2)
    gap5 = jnp.zeros((local_count, 5, node_count), F32)
    coeff_rows = jnp.concatenate((high, gap5, low, gap5), axis=1).astype(BF16)
    least = jnp.min(node_coords, axis=2)
    most = jnp.max(node_coords, axis=2)
    centre = 0.5 * (least + most)
    nodes = node_coords - centre[:, :, None]
    near = [-32.0 * piece for piece in outer_split(nodes, 3)]
    square = [16.0 * p for p in outer_split(jnp.sum(nodes * nodes, axis=1, keepdims=True), 3)]
    sixteen = jnp.full((local_count, 3, node_count), 16.0, F32)
    rows = [near[0]] * 3 + [near[1]] * 2 + [near[2], sixteen] + square
    rows.append(jnp.zeros((local_count, 8, node_count), F32))
    node_rows = jnp.concatenate(rows, axis=1).astype(BF16)
    table = jnp.concatenate((least, most, centre), axis=1)
    table = jnp.concatenate(outer_split(table, 3), axis=0).astype(BF16)
    table = jnp.pad(table, ((0, LANES - table.shape[0]), (0, LANES - table.shape[1])))

    id_source = arrived
    force = None
    backs = []
    for part in range(PARTS):
        following = None
        if part + 1 < PARTS:
            packed = pl.pallas_call(
                functools.partial(next_pack_kernel, part + 1),
                out_shape=jax.ShapeDtypeStruct((devices, 6 * GROUP, LANES), F32),
                in_specs=[smem(), vmem(), vmem()],
                out_specs=vmem(),
                name=f"pack_{part + 1}",
            )(pair_of, points, loads)
            packed, arrived, table, node_rows, coeff_rows = lax.optimization_barrier(
                (packed, arrived, table, node_rows, coeff_rows)
            )
            if part == 0:
                id_source = arrived
            following = exchange(packed)
        values, force = couple(part, id_source, arrived, table, node_rows, coeff_rows, force)
        backs.append(exchange(values))
        arrived = following

    point_disp = pl.pallas_call(
        unpack_kernel,
        out_shape=jax.ShapeDtypeStruct((3, tile_total, width), F32),
        in_specs=[smem()] + [vmem()] * (PARTS + 1),
        out_specs=vmem(),
        scratch_shapes=[pltpu.VMEM((3, pair_total + 8, width), F32)],
        name="unpack",
    )(pair_of, *backs, pu_level)
    return jnp.transpose(point_disp, (1, 0, 2)), jnp.transpose(force, (1, 0, 2))


def solution(mesh):
    placed = (
        P(AXES, None, None),
        P(AXES, None, None),
        P(AXES, None),
        P(AXES, None, None),
        P(AXES, None, None),
        P(AXES, None, None),
        P(AXES, None, None),
    )
    return jax.shard_map(
        on_device,
        mesh=mesh,
        in_specs=placed,
        out_specs=(P(AXES, None, None), P(AXES, None, None)),
        check_vma=False,
    )
```

```python
import functools

import jax
import jax.numpy as jnp
from jax import lax
from jax.experimental import pallas as pl
from jax.experimental.pallas import tpu as pltpu
from jax.sharding import PartitionSpec as P

CAP = 8
PARTS = 2
SHARE = CAP // PARTS
GROUP = 8
BATCH = 128
CHUNK = 256
TEAM = 4
WINDOW = 112
LANES = 128
AXES = ("row", "col")
NT = (((1,), (1,)), ((), ()))
F32 = jnp.float32
BF16 = jnp.bfloat16


def rounded(x):
    return x.astype(BF16).astype(F32)


def split2(x):
    high = rounded(x)
    return high, rounded(x - high)


def split3(x):
    high = rounded(x)
    rest = x - high
    middle = rounded(rest)
    return high, middle, rounded(rest - middle)


def outer_split(x, parts):
    pieces = []
    for _ in range(parts):
        piece = lax.reduce_precision(x, 8, 7)
        pieces.append(piece)
        x = x - piece
    return pieces


def tile_weights(levels):
    levels = levels.astype(F32) + 1.0
    return levels / jnp.sum(levels, axis=0, keepdims=True)


def iota(shape, axis):
    return lax.broadcasted_iota(jnp.int32, shape, axis)


def as_bf16(mask):
    return mask.astype(F32).astype(BF16)


def copy_slots(part, pair_of, points, loads, out):
    devices = out.shape[0]
    halves = points.shape[2] // LANES
    kslots = loads.shape[1] // points.shape[1]

    @pl.loop(0, devices)
    def _(d):
        for j in range(SHARE):
            pair = jnp.maximum(pair_of[d * CAP + part * SHARE + j], 0)
            tile = pair // kslots
            for c in range(6):
                whole = points[c, pl.ds(tile, 1), :] if c < 3 else loads[c - 3, pl.ds(pair, 1), :]
                for h in range(halves):
                    row = c * GROUP + h * SHARE + j
                    out[d, row : row + 1, :] = whole[:, h * LANES : (h + 1) * LANES]


def first_pack_kernel(local_count, full, ids, points, force, level, out, loads, pair_of, count):
    devices = out.shape[0]
    tiles, kslots = level.shape[0], level.shape[1]

    @pl.loop(0, devices)
    def _(d):
        count[d] = 0
        if not full:
            out[d, 6 * GROUP : 7 * GROUP, :] = jnp.full((CAP, LANES), -1.0, F32)
            for j in range(CAP):
                pair_of[d * CAP + j] = -1

    @pl.loop(0, tiles)
    def _(t):
        weights = tile_weights(level[t])
        for c in range(3):
            where = pl.ds(pl.multiple_of(t * kslots, kslots), kslots)
            loads[c, where, :] = weights * (force[c, pl.ds(t, 1), :] * (1.0 / 256.0))
        for k in range(kslots):
            pair = t * kslots + k
            cluster = ids[pair]
            d = cluster // local_count
            j = count[d]
            count[d] = j + 1
            pair_of[d * CAP + j] = pair
            own = (cluster - d * local_count).astype(F32)
            out[d, pl.ds(6 * GROUP + j, 1), :] = jnp.full((1, LANES), own)

    copy_slots(0, pair_of, points, loads, out)


def next_pack_kernel(part, pair_of, points, loads, out):
    copy_slots(part, pair_of, points, loads, out)


def unpack_kernel(pair_of, *refs):
    backs, level, out, rows = refs[:PARTS], refs[PARTS], refs[PARTS + 1], refs[PARTS + 2]
    tiles, kslots = level.shape[0], level.shape[1]
    halves = out.shape[2] // LANES
    devices = backs[0].shape[0]

    @pl.loop(0, devices)
    def _(d):
        for slot in range(CAP):
            pair = pair_of[d * CAP + slot]
            pair = jnp.where(pair < 0, tiles * kslots, pair)
            back, j = backs[slot // SHARE], slot % SHARE
            for c in range(3):
                pieces = [
                    back[d, c * GROUP + h * SHARE + j : c * GROUP + h * SHARE + j + 1, :]
                    for h in range(halves)
                ]
                rows[c, pl.ds(pair, 1), :] = jnp.concatenate(pieces, axis=1)

    @pl.loop(0, tiles)
    def _(t):
        weights = tile_weights(level[t])
        where = pl.ds(pl.multiple_of(t * kslots, kslots), kslots)
        for c in range(3):
            out[c, pl.ds(t, 1), :] = jnp.sum(weights * rows[c, where, :], axis=0, keepdims=True)


def couple_kernel(part, *refs):
    refs = list(refs)
    first, last = part == 0, part == PARTS - 1
    id_tiles, arrived, table, node_rows, coeff_rows = refs[:5]
    del refs[:5]
    earlier_force = None if first else refs.pop(0)
    id_row = id_tiles.shape[1] - CAP + part * SHARE
    values, node_force = refs[:2]
    (
        rank,
        id_rows,
        boxes,
        rows,
        packed,
        found_rows,
        even,
        odd,
        slot_plan_v,
        cluster_plan_v,
        slot_plan,
        cluster_plan,
        cluster_of,
        force_sum,
        sems,
    ) = refs[2:]
    sources = arrived.shape[0]
    batch = sources * SHARE
    groups = batch // GROUP
    per_group = GROUP // SHARE
    halves = GROUP // SHARE
    width = halves * LANES
    clusters = node_rows.shape[0]
    step = pl.program_id(0)

    @pl.when(step == 0)
    def _():
        if first:
            force_sum[...] = jnp.zeros_like(force_sum)
        else:
            force_sum[...] = earlier_force[...]

    def group_rows(g):
        return pl.ds(pl.multiple_of(g * GROUP, GROUP), GROUP)

    @pl.loop(0, groups)
    def _(g):
        id_rows[group_rows(g), :] = jnp.concatenate(
            [
                id_tiles[g * per_group + i, id_row : id_row + SHARE, :]
                for i in range(per_group)
            ],
            axis=0,
        )

    lane = iota((1, LANES), 1)
    own = id_rows[...]
    thrice = (own == (lane % clusters).astype(F32)) & (lane < 3 * clusters)
    boxes[...] = jnp.dot(as_bf16(thrice), table[...], preferred_element_type=F32)

    def slot_tiles(box, i):
        return jnp.concatenate([box[i * SHARE : (i + 1) * SHARE]] * halves, axis=0)

    @pl.loop(0, groups)
    def _(g):
        found = []
        for i in range(per_group):
            d = g * per_group + i
            box = slot_tiles(boxes[group_rows(g), :], i)
            gap = jnp.where(slot_tiles(id_rows[group_rows(g), :], i) < 0.0, 4.0, 0.0)
            for c in range(3):
                x = arrived[d, c * GROUP : (c + 1) * GROUP, :]
                side = jnp.maximum(box[:, c : c + 1] - x, x - box[:, 3 + c : 4 + c])
                side = jnp.maximum(side, 0.0)
                gap = gap + side * side
            found.append(jnp.where(gap < 1.0002, 1.0, 0.0))
        for h in range(halves):
            rank[group_rows(g), h * LANES : (h + 1) * LANES] = jnp.concatenate(
                [tile[h * SHARE : (h + 1) * SHARE] for tile in found], axis=0
            )

    near = rank[...].astype(BF16)
    before = as_bf16(iota((width, width), 0) < iota((width, width), 1))
    earlier = jnp.dot(near, before, preferred_element_type=F32)
    rank[...] = jnp.where(near.astype(F32) > 0.5, earlier, -1e6)
    counts = lax.dot_general(jnp.ones((8, width), BF16), near, NT, preferred_element_type=F32)
    pick = as_bf16(iota((clusters, LANES), 0) == iota((clusters, LANES), 1))
    hits = lax.dot_general(
        pick, as_bf16(own == lane.astype(F32)), NT, preferred_element_type=F32
    )
    hit_counts = hits * counts[0:1]
    before_slot = as_bf16(iota((batch, batch), 0) < iota((batch, batch), 1))
    slot_start = jnp.dot(hit_counts.astype(BF16), before_slot, preferred_element_type=F32)
    totals = jnp.sum(hit_counts, axis=1, keepdims=True)
    chunks = jnp.floor((totals + (CHUNK - 1)) * (1.0 / CHUNK))
    chunks = jnp.broadcast_to(chunks, (clusters, LANES))
    before_cluster = as_bf16(iota((clusters, clusters), 1) < iota((clusters, clusters), 0))
    first_chunk = jnp.dot(before_cluster, chunks.astype(BF16), preferred_element_type=F32)
    offset = jnp.sum(hits * (slot_start + first_chunk[:, 0:1] * CHUNK), axis=0, keepdims=True)
    slot_plan_v[0:1, :] = offset.astype(jnp.int32)
    slot_plan_v[1:2, :] = counts[0:1].astype(jnp.int32)
    cluster_plan_v[...] = jnp.where(lane == 0, first_chunk, chunks).astype(jnp.int32)
    copies = [
        pltpu.make_async_copy(slot_plan_v, slot_plan, sems.at[0]),
        pltpu.make_async_copy(cluster_plan_v, cluster_plan, sems.at[1]),
    ]
    for copy in copies:
        copy.start()
    for copy in copies:
        copy.wait()
    total_chunks = cluster_plan[clusters - 1, 0] + cluster_plan[clusters - 1, 1]

    @pl.loop(0, clusters)
    def _(c):
        @pl.loop(0, cluster_plan[c, 1])
        def _(j):
            cluster_of[cluster_plan[c, 0] + j] = c

    def chunk_rows(j):
        return pl.ds(pl.multiple_of(j * CHUNK, CHUNK), CHUNK)

    @pl.loop(0, total_chunks + 3)
    def _(j):
        packed[chunk_rows(j), :] = jnp.zeros((CHUNK, LANES), F32)

    for extra in range(2):
        found_rows[chunk_rows(total_chunks + extra), 0:16] = jnp.zeros((CHUNK, 16), F32)

    for extra in range(3):
        cluster_of[total_chunks + extra] = 0

    target = iota((WINDOW, 1), 0).astype(F32)

    def places_of(team):
        places = []
        for i in range(TEAM * GROUP):
            slot = team * (TEAM * GROUP) + i
            start = slot_plan[0, slot]
            base = (start // 8) * 8
            lead = start - base
            blocks = (lead + slot_plan[1, slot] + (WINDOW - 1)) // WINDOW
            places.append((rank[pl.ds(slot, 1), :], base, lead, blocks))
        most = places[0][3]
        for place in places[1:]:
            most = jnp.maximum(most, place[3])
        return places, most

    def selection(place, block):
        shift = (place[2] - block * WINDOW).astype(F32)
        return jnp.where(place[0] + shift == target, 1.0, 0.0).astype(BF16)

    def window_of(place, block):
        return pl.ds(pl.multiple_of(place[1] + block * WINDOW, 8), WINDOW)

    @pl.loop(0, groups // TEAM)
    def _(team):
        for i in range(TEAM * per_group):
            d = team * (TEAM * per_group) + i
            box = slot_tiles(boxes[group_rows(team * TEAM + i // per_group), :], i % per_group)
            x = [
                arrived[d, c * GROUP : (c + 1) * GROUP, :] - box[:, 6 + c : 7 + c] for c in range(3)
            ]
            parts = [split3(v) for v in x]
            square = split3(x[0] * x[0] + x[1] * x[1] + x[2] * x[2])
            loads = [split2(arrived[d, (3 + c) * GROUP : (4 + c) * GROUP, :]) for c in range(3)]
            column = [parts[c][p] for p in (0, 1, 2, 0, 1, 0) for c in range(3)]
            column += list(square) + [jnp.ones_like(x[0])] * 3
            column += [loads[c][p] for p in range(2) for c in range(3)]
            column += [jnp.zeros_like(x[0])] * 2
            for n, tile in enumerate(column):
                rows[i, n * GROUP : (n + 1) * GROUP, :] = tile
        places, most = places_of(team)

        def gathered(i, block):
            source = rows.at[i // SHARE]
            pieces = [
                source[pl.ds(h * SHARE + i % SHARE, 32, stride=GROUP), :] for h in range(halves)
            ]
            return lax.dot_general(
                selection(places[i], block),
                jnp.concatenate(pieces, axis=1).astype(BF16),
                NT,
                preferred_element_type=F32,
            )

        moved = [gathered(i, 0) for i in range(TEAM * GROUP)]
        for i in range(TEAM * GROUP):
            packed[window_of(places[i], 0), 0:32] += moved[i]

        @pl.when(most > 1)
        def _():
            for i in range(TEAM * GROUP):

                @pl.loop(1, places[i][3])
                def _(block):
                    packed[window_of(places[i], block), 0:32] += gathered(i, block)

    def distances(j, squares):
        squares[...] = jnp.dot(
            packed[chunk_rows(j), 0:32].astype(BF16),
            node_rows[cluster_of[j]],
            preferred_element_type=F32,
        )

    def contract(j, squares):
        c = cluster_of[j]
        square = jnp.maximum(squares[...], 1e-30)
        rest = jnp.maximum(4.0 - square * lax.rsqrt(square), 0.0)
        rest2 = rest * rest
        kernel = (rest2 * rest2) * (5.0 - rest)
        high = kernel.astype(BF16)
        low = (kernel - high.astype(F32)).astype(BF16)
        loads = jnp.transpose(packed[chunk_rows(j), :])[24:32].astype(BF16)
        found_rows[chunk_rows(j), 0:16] = lax.dot_general(
            high, coeff_rows[c], NT, preferred_element_type=F32
        ) + lax.dot_general(low, coeff_rows[c], NT, preferred_element_type=F32)
        force_sum[c] += jnp.dot(loads, high, preferred_element_type=F32) + jnp.dot(
            loads, low, preferred_element_type=F32
        )

    distances(0, even)

    @pl.loop(0, (total_chunks + 1) // 2)
    def _(j):
        distances(2 * j + 1, odd)
        contract(2 * j, even)
        distances(2 * j + 2, even)
        contract(2 * j + 1, odd)

    @pl.loop(0, groups // TEAM)
    def _(team):
        places, most = places_of(team)

        def spread(i, block):
            rows_t = jnp.transpose(found_rows[window_of(places[i], block), :])
            high, middle, low = split3(rows_t[0:8] + rows_t[8:16])
            stacked = jnp.concatenate([high, middle, low], axis=0).astype(BF16)
            moved = jnp.dot(stacked, selection(places[i], block), preferred_element_type=F32)
            return moved[0:8] + moved[8:16] + moved[16:24]

        def pieces_of(i, found):
            d = team * (TEAM * per_group) + i // SHARE
            for c in range(3):
                for h in range(halves):
                    row = c * GROUP + h * SHARE + i % SHARE
                    yield d, row, found[c : c + 1, h * LANES : (h + 1) * LANES]

        spreads = [spread(i, 0) for i in range(TEAM * GROUP)]
        for i in range(TEAM * GROUP):
            for d, row, piece in pieces_of(i, spreads[i]):
                values[d, row : row + 1, :] = piece

        @pl.when(most > 1)
        def _():
            for i in range(TEAM * GROUP):

                @pl.loop(1, places[i][3])
                def _(block):
                    for d, row, piece in pieces_of(i, spread(i, block)):
                        values[d, row : row + 1, :] += piece

    @pl.when(step == pl.num_programs(0) - 1)
    def _():
        if last:
            for c in range(clusters):
                both = force_sum[c]
                for i in range(3):
                    node_force[i, c : c + 1, :] = both[i : i + 1] + both[3 + i : 4 + i]
        else:
            node_force[...] = force_sum[...]


def vmem():
    return pl.BlockSpec(memory_space=pltpu.VMEM)


def smem():
    return pl.BlockSpec(memory_space=pltpu.SMEM)


def couple(part, id_source, arrived, table, node_rows, coeff_rows, earlier_force):
    devices = arrived.shape[0]
    clusters, _, nodes = node_rows.shape
    batch = min(BATCH, devices * SHARE)
    sources = batch // SHARE
    width = GROUP // SHARE * LANES
    last = part == PARTS - 1
    steps = devices * SHARE // batch
    force_shape = (3, clusters, nodes) if last else (clusters, 8, nodes)
    room = batch * width + clusters * CHUNK + 3 * CHUNK + 2 * WINDOW
    extra = () if earlier_force is None else (earlier_force,)
    pairs = devices * SHARE * width // 4
    return pl.pallas_call(
        functools.partial(couple_kernel, part),
        grid=(steps,),
        out_shape=(
            jax.ShapeDtypeStruct((devices, 3 * GROUP, LANES), F32),
            jax.ShapeDtypeStruct(force_shape, F32),
        ),
        in_specs=[
            vmem() if steps == 1 else pl.BlockSpec((sources, GROUP, LANES), lambda i: (i, 6, 0)),
            vmem() if steps == 1 else pl.BlockSpec((sources, 6 * GROUP, LANES), lambda i: (i, 0, 0)),
            vmem(),
            vmem(),
            vmem(),
        ]
        + [vmem() for _ in extra],
        out_specs=(
            vmem() if steps == 1 else pl.BlockSpec((sources, 3 * GROUP, LANES), lambda i: (i, 0, 0)),
            vmem() if steps == 1 else pl.BlockSpec(force_shape, lambda i: (0, 0, 0)),
        ),
        scratch_shapes=[
            pltpu.VMEM((batch, width), F32),
            pltpu.VMEM((batch, LANES), F32),
            pltpu.VMEM((batch, LANES), F32),
            pltpu.VMEM((TEAM * GROUP // SHARE, 32 * GROUP, LANES), F32),
            pltpu.VMEM((room, LANES), F32),
            pltpu.VMEM((room, LANES), F32),
            pltpu.VMEM((CHUNK, nodes), F32),
            pltpu.VMEM((CHUNK, nodes), F32),
            pltpu.VMEM((8, batch), jnp.int32),
            pltpu.VMEM((clusters, LANES), jnp.int32),
            pltpu.SMEM((8, batch), jnp.int32),
            pltpu.SMEM((clusters, LANES), jnp.int32),
            pltpu.SMEM((room // CHUNK + 4,), jnp.int32),
            pltpu.VMEM((clusters, 8, nodes), F32),
            pltpu.SemaphoreType.DMA((2,)),
        ],
        compiler_params=pltpu.CompilerParams(vmem_limit_bytes=52 * 1024 * 1024),
        cost_estimate=pl.CostEstimate(
            flops=pairs * nodes * 80, bytes_accessed=arrived.size * 6, transcendentals=pairs * nodes
        ),
        name=f"couple_{part}",
    )(id_source, arrived, table, node_rows, coeff_rows, *extra)


def exchange(x):
    return lax.all_to_all(x, AXES, split_axis=0, concat_axis=0, tiled=True)


def on_device(point_coords, fluid_force, tile_clusters, pu_level, node_coords, node_disp, inverse):
    highest = lax.Precision.HIGHEST
    devices = lax.axis_size(AXES)
    slot_total = devices * CAP
    tile_total, kslots = tile_clusters.shape
    pair_total = tile_total * kslots
    local_count, _, node_count = node_coords.shape
    width = point_coords.shape[2]
    points = jnp.transpose(point_coords, (1, 0, 2))

    outgoing, loads, pair_of = pl.pallas_call(
        functools.partial(first_pack_kernel, local_count, pair_total == slot_total),
        out_shape=(
            jax.ShapeDtypeStruct((devices, 7 * GROUP, LANES), F32),
            jax.ShapeDtypeStruct((3, pair_total, width), F32),
            jax.ShapeDtypeStruct((slot_total,), jnp.int32),
        ),
        in_specs=[smem(), vmem(), vmem(), vmem()],
        out_specs=(vmem(), vmem(), smem()),
        scratch_shapes=[pltpu.SMEM((devices,), jnp.int32)],
        name="pack_0",
    )(tile_clusters.reshape(-1), points, jnp.transpose(fluid_force, (1, 0, 2)), pu_level)
    arrived = exchange(outgoing)

    coeffs = jnp.einsum("cin,cnm->cim", node_disp, inverse, precision=highest) * (1.0 / 256.0)
    high, low = outer_split(coeffs, 2)
    gap5 = jnp.zeros((local_count, 5, node_count), F32)
    coeff_rows = jnp.concatenate((high, gap5, low, gap5), axis=1).astype(BF16)
    least = jnp.min(node_coords, axis=2)
    most = jnp.max(node_coords, axis=2)
    centre = 0.5 * (least + most)
    nodes = node_coords - centre[:, :, None]
    near = [-32.0 * piece for piece in outer_split(nodes, 3)]
    square = [16.0 * p for p in outer_split(jnp.sum(nodes * nodes, axis=1, keepdims=True), 3)]
    sixteen = jnp.full((local_count, 3, node_count), 16.0, F32)
    rows = [near[0]] * 3 + [near[1]] * 2 + [near[2], sixteen] + square
    rows.append(jnp.zeros((local_count, 8, node_count), F32))
    node_rows = jnp.concatenate(rows, axis=1).astype(BF16)
    table = jnp.concatenate((least, most, centre), axis=1)
    table = jnp.concatenate(outer_split(table, 3), axis=0).astype(BF16)
    table = jnp.pad(table, ((0, LANES - table.shape[0]), (0, LANES - table.shape[1])))

    id_source = arrived
    force = None
    backs = []
    for part in range(PARTS):
        following = None
        if part + 1 < PARTS:
            packed = pl.pallas_call(
                functools.partial(next_pack_kernel, part + 1),
                out_shape=jax.ShapeDtypeStruct((devices, 6 * GROUP, LANES), F32),
                in_specs=[smem(), vmem(), vmem()],
                out_specs=vmem(),
                name=f"pack_{part + 1}",
            )(pair_of, points, loads)
            packed, arrived, table, node_rows, coeff_rows = lax.optimization_barrier(
                (packed, arrived, table, node_rows, coeff_rows)
            )
            if part == 0:
                id_source = arrived
            following = exchange(packed)
        values, force = couple(part, id_source, arrived, table, node_rows, coeff_rows, force)
        backs.append(exchange(values))
        arrived = following

    point_disp = pl.pallas_call(
        unpack_kernel,
        out_shape=jax.ShapeDtypeStruct((3, tile_total, width), F32),
        in_specs=[smem()] + [vmem()] * (PARTS + 1),
        out_specs=vmem(),
        scratch_shapes=[pltpu.VMEM((3, pair_total + 8, width), F32)],
        name="unpack",
    )(pair_of, *backs, pu_level)
    return jnp.transpose(point_disp, (1, 0, 2)), jnp.transpose(force, (1, 0, 2))


def solution(mesh):
    placed = (
        P(AXES, None, None),
        P(AXES, None, None),
        P(AXES, None),
        P(AXES, None, None),
        P(AXES, None, None),
        P(AXES, None, None),
        P(AXES, None, None),
    )
    return jax.shard_map(
        on_device,
        mesh=mesh,
        in_specs=placed,
        out_specs=(P(AXES, None, None), P(AXES, None, None)),
        check_vma=False,
    )
```
